32 devices in a mesh: dp: 4 (over x, core), param: 8 (over z, y).
Axes of the slice: x: 2, y: 2, z: 4, core: 2. Of those that a mesh axis runs over, the one named last changes fastest.
Arguments:
- train_grads: bfloat16 [3584, 212992], P('dp', 'param'), as said below
- query_grads: bfloat16 [128, 212992], P('dp', 'param'), as said below
Outputs:
- scores: float32 [128, 3584], P('param', 'dp')
Inputs may be any that keep to these rules, and one draw needn't show every extreme that they name: `train_grads`: finite real values. `query_grads`: finite real values.
All inputs are finite; a program needn't handle non-finite values.
Results may differ from the reference program's by a relative error of at most 0.0003.
Values may be sent and summed in bfloat16 or wider, within the bound.
A program may use at most 128 MiB of HBM per device.

```python
import math
import jax
import jax.numpy as jnp
from jax import lax

TR_DEV = 896
GRAD = 212992
NTR = 3584
NQ = 128
N_DP = 4


latent_count = 256


decay_power = 0.35


def shared_basis(key):
    base = jax.random.fold_in(key, 7)
    spread = jax.random.uniform(jax.random.fold_in(base, 1), (GRAD,), jnp.float32)
    column_scale = jnp.exp(math.log(10.0) * spread) * (1.0 + 2.0 * jnp.arange(GRAD, dtype=jnp.float32) / GRAD)
    basis = jax.random.normal(jax.random.fold_in(base, 2), (latent_count, GRAD), jnp.float32)
    return (column_scale, basis)


def make_grads(key, salt, row_count):
    column_scale, basis = shared_basis(key)
    inner = jax.random.fold_in(key, salt)
    decay = jnp.power(jnp.arange(latent_count, dtype=jnp.float32) + 1.0, -decay_power)
    decay = decay / jnp.sqrt(jnp.sum(decay * decay))
    weights = jax.random.normal(jax.random.fold_in(inner, 1), (row_count, latent_count), jnp.float32) * decay[None, :]
    noise = jax.random.normal(jax.random.fold_in(inner, 2), (row_count, GRAD), jnp.float32)
    spread = jax.random.uniform(jax.random.fold_in(inner, 3), (row_count,), jnp.float32)
    mixed = jnp.dot(weights, basis) + 0.5 * noise
    row_scale = jnp.exp(math.log(10.0) * spread)
    return (row_scale[:, None] * column_scale[None, :] * mixed).astype(jnp.bfloat16)


def draw_train_grads(key, part):
    return make_grads(key, 11, NTR)


def draw_query_grads(key, part):
    return make_grads(key, 13, NQ)


def setup_inputs(seed: int = 0) -> dict:
    splits = jax.random.split(jax.random.key(seed), 3)
    return {
        "train_grads": draw_train_grads(jax.random.fold_in(splits[2], 71), 0),
        "query_grads": draw_query_grads(jax.random.fold_in(splits[2], 71), 0),
    }


epsilon = 1e-06

def reference(train_grads, query_grads):
    query_norm = lax.optimization_barrier(jnp.sum(jnp.square(query_grads.astype(jnp.float32)), axis=1))
    blocks = train_grads.reshape(N_DP, TR_DEV, GRAD)

    def one_block(block):
        products = lax.dot_general(query_grads, block, (((1,), (1,)), ((), ())), preferred_element_type=jnp.float32)
        block_norm = lax.optimization_barrier(jnp.sum(jnp.square(block.astype(jnp.float32)), axis=1))
        return (products, block_norm)
    products, train_norm = lax.map(one_block, blocks)
    products = jnp.transpose(products, (1, 0, 2)).reshape(NQ, NTR)
    train_norm = train_norm.reshape(NTR)
    return products * lax.rsqrt(query_norm + epsilon)[:, None] * lax.rsqrt(train_norm + epsilon)[None, :]
```

```python
import functools

import jax
import jax.numpy as jnp
from jax import lax
from jax.experimental import pallas as pl
from jax.experimental.pallas import tpu as pltpu
from jax.sharding import PartitionSpec as P

epsilon = 1e-06
lanes = 128
sublanes = 8
max_chunk = 2048
block_rows = 256
train_width = 1024
x_width = 1024


def chunk_width(width):
    best = lanes
    for tiles in range(1, max_chunk // lanes + 1):
        if width % (tiles * lanes) == 0:
            best = tiles * lanes
    return best


def column_plan(total):
    base = chunk_width(total)
    chunks = total // base
    pairs = (chunks - 1) // 2
    first = [(2 * base * g, 2 * base) for g in range(pairs)]
    first.append((2 * base * pairs, total - 2 * base * pairs))
    looped = max(pairs - 1, 0)
    second = [(2 * base * g, 2 * base) for g in range(looped)]
    at = 2 * base * looped
    fine = 1024 if base % 1024 == 0 else base
    while total - at > 4 * fine:
        size = min(base, total - at - 4 * fine)
        second.append((at, size))
        at += size
    while at < total:
        size = min(fine, total - at)
        second.append((at, size))
        at += size
    return base, pairs, looped, first, second


def nt_dot(a, b):
    return lax.dot_general(a, b, (((1,), (1,)), ((), ())), preferred_element_type=jnp.float32)


def kernel(
    cfg, train_hbm, query_hbm, out_ref,
    train, first_q, second_q, first_sum, second_sum, norm_sum, parts, norm_parts, query_sum, query_scales, scale,
    train_sem, self_sem, x_send, first_recv, second_recv, mate_send, mate_recv,
    fwd_send, first_fwd, second_fwd, part_send, part_recv, norm_send, norm_recv,
    query_send, query_recv, known,
):
    chips, params, total, rows, unit, count, owned, piece, plan = cfg
    base, pairs, looped, first_plan, second_plan = plan
    dp = lax.axis_index("dp")
    me = lax.axis_index("param")
    chip, core = dp // 2, lax.rem(dp, 2)
    mate = chip * 2 + (1 - core)
    cores = 2 * chips
    near = 2 * rows
    x_recv = (first_recv, second_recv)
    fwd_recv = (first_fwd, second_fwd)

    def bytes_wait(ref, sem):
        pltpu.make_async_copy(ref, ref, sem).wait()

    def columns(group, i):
        plan_of = first_plan if group == 0 else second_plan
        if isinstance(i, int):
            start, size = plan_of[i]
            return pl.ds(start, size)
        return pl.ds(pl.multiple_of(i * 2 * base, 2 * base), 2 * base)

    def split(start, size, width):
        return [pl.ds(start + k, min(width, size - k)) for k in range(0, size, width)]

    def train_copies(i):
        return [
            pltpu.make_async_copy(train_hbm.at[:, cols], train.at[:, cols], train_sem.at[i])
            for cols in split(*first_plan[i], train_width)
        ]

    def self_copies(i):
        return [
            pltpu.make_async_copy(query_hbm.at[:, cols], first_q.at[pl.ds(0, rows), cols], self_sem.at[i])
            for cols in split(*first_plan[i], base)
        ]

    def wait_train(i):
        bytes_wait(query_hbm.at[:, columns(0, i)], self_sem.at[i])
        bytes_wait(train.at[:, columns(0, i)], train_sem.at[i])

    def mate_copies(i):
        return [
            pltpu.make_async_remote_copy(
                src_ref=query_hbm.at[:, cols],
                dst_ref=first_q.at[pl.ds(rows, rows), cols],
                send_sem=mate_send.at[0],
                recv_sem=mate_recv.at[0],
                device_id={"dp": mate},
            )
            for cols in split(*first_plan[i], base)
        ]

    def slot(group, i, place):
        if group == 0:
            return first_q.at[pl.ds(near + unit * place, unit), columns(0, i)]
        return second_q.at[pl.ds(unit * place, unit), columns(1, i)]

    def x_copies(group, i, d):
        start = pl.multiple_of(lax.rem(group + core, 2) * unit, unit)
        place = pl.ds((near if group == 0 else 0) + unit * 2 * (d - 1), unit)
        dst = first_q if group == 0 else second_q
        return [
            pltpu.make_async_remote_copy(
                src_ref=query_hbm.at[pl.ds(start, unit), cols],
                dst_ref=dst.at[place, cols],
                send_sem=x_send.at[d - 1],
                recv_sem=x_recv[group].at[d - 1, i],
                device_id={"dp": lax.rem(chip + d, chips) * 2 + core},
            )
            for cols in split(*(first_plan if group == 0 else second_plan)[i], x_width)
        ]

    def fwd_copy(group, i, d):
        return pltpu.make_async_remote_copy(
            src_ref=slot(group, i, 2 * (d - 1)),
            dst_ref=slot(group, i, 2 * (d - 1) + 1),
            send_sem=fwd_send.at[0],
            recv_sem=fwd_recv[group].at[d - 1, i],
            device_id={"dp": mate},
        )

    def pump(group, i):
        for d in range(1, chips):
            bytes_wait(slot(group, i, 2 * (d - 1)), x_recv[group].at[d - 1, i])
            fwd_copy(group, i, d).start()

    def arrive(group, i):
        for d in range(1, chips):
            fwd_copy(group, i, d).wait_recv()

    def piece_list(group):
        out = []
        if group == 0:
            for source, at in ((dp, 0), (mate, rows)):
                for r in range(0, rows, piece):
                    out.append((first_sum, at + r, source * rows + r))
        for d in range(1, chips):
            other = lax.rem(chip - d + chips, chips)
            for k in range(2):
                from_core = core if k == 0 else 1 - core
                start = lax.rem(group + from_core, 2) * unit
                at = unit * (2 * (d - 1) + k)
                for r in range(0, unit, piece):
                    row = (other * 2 + from_core) * rows + start + r
                    if group == 0:
                        out.append((first_sum, near + at + r, row))
                    else:
                        out.append((second_sum, at + r, row))
        return out

    def send_parts(items):
        for buffer, at, row in items:
            owner, offset = row // owned, lax.rem(row, owned)
            place = parts.at[me, pl.ds(pl.multiple_of(offset, piece), piece), :]
            copy = pltpu.make_async_remote_copy(
                src_ref=buffer.at[pl.ds(at, piece), :],
                dst_ref=place,
                send_sem=part_send.at[0],
                recv_sem=part_recv.at[0],
                device_id={"param": owner},
            )

            @pl.when(owner != me)
            def _():
                copy.start()

            @pl.when(owner == me)
            def _():
                place[...] = buffer[pl.ds(at, piece), :]

    def norm_copy(j):
        return pltpu.make_async_remote_copy(
            src_ref=norm_parts.at[me],
            dst_ref=norm_parts.at[me],
            send_sem=norm_send.at[0],
            recv_sem=norm_recv.at[0],
            device_id={"param": lax.rem(me + j, params)},
        )

    def query_copy(j):
        return pltpu.make_async_remote_copy(
            src_ref=query_scales,
            dst_ref=query_scales,
            send_sem=query_send.at[0],
            recv_sem=query_recv.at[0],
            device_id={"dp": lax.rem(dp + j, cores)},
        )

    pairmate = me + 1 - 2 * lax.rem(me, 2)
    neighbours = (pairmate, lax.rem(me + 2, params), lax.rem(me + params - 2, params))
    stages = known.shape[0]

    for i in range(len(first_plan)):
        for copy in self_copies(i) + train_copies(i):
            copy.start()

    barrier = pltpu.get_barrier_semaphore()
    for j in range(1, cores):
        pl.semaphore_signal(barrier, inc=1, device_id={"dp": lax.rem(dp + j, cores)})
    for other in neighbours:
        pl.semaphore_signal(barrier, inc=1, device_id={"param": other})
    pl.semaphore_wait(barrier, cores - 1 + len(neighbours))

    for other in neighbours:
        pl.semaphore_signal(known.at[0], inc=1, device_id={"param": other})
    for i in range(len(first_plan)):
        for d in range(1, chips):
            for copy in x_copies(0, i, d):
                copy.start()
        for copy in mate_copies(i):
            copy.start()
    for i in range(len(second_plan)):
        for d in range(1, chips):
            for copy in x_copies(1, i, d):
                copy.start()

    first_sum[...] = jnp.zeros_like(first_sum)
    second_sum[...] = jnp.zeros_like(second_sum)
    norm_sum[...] = jnp.zeros_like(norm_sum)

    query_sum[...] = jnp.zeros_like(query_sum)

    def next_round(stage):
        pl.semaphore_wait(known.at[stage], len(neighbours))
        if stage + 1 < stages:
            for other in neighbours:
                pl.semaphore_signal(known.at[stage + 1], inc=1, device_id={"param": other})

    def multiply(sums, q_ref, start, width, norms):
        if not isinstance(start, int):
            start = pl.multiple_of(start, base)
        q = q_ref[:, pl.ds(start, width)]
        if norms:
            acc = query_sum[...]
            for k in range(0, width, lanes):
                x = q[:rows, k : k + lanes].astype(jnp.float32)
                acc = acc + x * x
            query_sum[...] = acc
        for r in range(0, count, block_rows):
            size = min(block_rows, count - r)
            t = train[pl.ds(r, size), pl.ds(start, width)]
            sums[:, pl.ds(r, size)] += nt_dot(q, t)
            if norms:
                for s in range(0, size, lanes):
                    acc = norm_sum[pl.ds(r + s, lanes), :]
                    for k in range(0, width, lanes):
                        x = t[s : s + lanes, k : k + lanes].astype(jnp.float32)
                        acc = acc + x * x
                    norm_sum[pl.ds(r + s, lanes), :] = acc

    bytes_wait(query_hbm, mate_recv.at[0])
    pump(0, 0)

    @pl.loop(0, pairs)
    def _(g):
        wait_train(g)
        arrive(0, g)
        multiply(first_sum, first_q, g * 2 * base, base, True)

        @pl.when(g + 1 < pairs)
        def _():
            pump(0, g + 1)

        @pl.when(g + 1 == pairs)
        def _():
            pump(0, pairs)

        multiply(first_sum, first_q, g * 2 * base + base, base, True)

        @pl.when(g == 0)
        def _():
            next_round(0)

    start, size = first_plan[pairs]
    wait_train(pairs)
    arrive(0, pairs)
    for at in range(start, start + size, base):
        multiply(first_sum, first_q, at, base, True)

    for stage in range(1, stages):
        next_round(stage)
    send_parts(piece_list(0))

    totals = [
        jnp.sum(norm_sum[pl.ds(r, lanes), :].T, axis=0, keepdims=True) for r in range(0, count, lanes)
    ]
    query_row = len(totals)
    square = jnp.concatenate([query_sum[...], jnp.zeros((lanes - rows, lanes), jnp.float32)], axis=0)
    totals.append(jnp.sum(square.T, axis=0, keepdims=True))
    spare = norm_parts.shape[1] - len(totals)
    if spare:
        totals.append(jnp.zeros((spare, lanes), jnp.float32))
    norm_parts[me] = jnp.concatenate(totals, axis=0)
    for j in range(1, params):
        norm_copy(j).start()

    first_row = me * owned
    source = first_row // rows

    def share_scales():
        bytes_wait(norm_parts.at[pl.ds(0, params - 1)], norm_send.at[0])
        bytes_wait(norm_parts.at[pl.ds(0, params - 1)], norm_recv.at[0])
        norm = norm_parts[0]
        for j in range(1, params):
            norm = norm + norm_parts[j]
        scale[...] = lax.rsqrt(norm + epsilon)

        @pl.when(dp == source)
        def _():
            query_scales[...] = jnp.broadcast_to(scale[query_row : query_row + 1, :], query_scales.shape)
            for j in range(1, cores):
                query_copy(j).start()

    pump(1, 0)
    if looped:
        @pl.loop(0, looped)
        def _(g):
            arrive(1, g)
            multiply(second_sum, second_q, g * 2 * base, base, False)

            @pl.when(g + 1 < looped)
            def _():
                pump(1, g + 1)

            @pl.when(g + 1 == looped)
            def _():
                pump(1, looped)

            multiply(second_sum, second_q, g * 2 * base + base, base, False)

            @pl.when(g == looped - 1)
            def _():
                share_scales()

    else:
        share_scales()

    last = len(second_plan) - 1
    for i in range(looped, last + 1):
        if i < last:
            pump(1, i + 1)
        arrive(1, i)
        multiply(second_sum, second_q, *second_plan[i], False)

    send_parts(piece_list(1))

    @pl.when(dp == source)
    def _():
        bytes_wait(norm_parts.at[pl.ds(0, cores - 1)], query_send.at[0])

    @pl.when(dp != source)
    def _():
        bytes_wait(query_scales, query_recv.at[0])

    pick = lax.broadcasted_iota(jnp.int32, (owned, lanes), 1) == (
        lax.broadcasted_iota(jnp.int32, (owned, lanes), 0) + lax.rem(first_row, rows)
    )
    query_scale = jnp.sum(jnp.where(pick, query_scales[0:1, :], 0.0), axis=1, keepdims=True)

    bytes_wait(query_hbm, mate_send.at[0])
    for d in range(1, chips):
        bytes_wait(query_hbm, x_send.at[d - 1])
    bytes_wait(second_q, fwd_send.at[0])

    bytes_wait(parts.at[pl.ds(0, params - 1)], part_recv.at[0])
    for k in range(count // lanes):
        at = slice(k * lanes, (k + 1) * lanes)
        products = parts[0, :, at]
        for j in range(1, params):
            products = products + parts[j, :, at]
        out_ref[:, at] = products * query_scale * scale[k : k + 1, :]

    bytes_wait(parts.at[pl.ds(0, params - 1)], part_send.at[0])


def solution(mesh):
    chips, params = mesh.shape["dp"] // 2, mesh.shape["param"]

    def per_device(train_grads, query_grads):
        count, total = train_grads.shape
        rows = query_grads.shape[0]
        unit = rows // 2
        cores = 2 * chips
        owned = rows * cores // params
        piece = min(unit, owned)
        far = 2 * (chips - 1) * unit
        plan = column_plan(total)
        _base, _pairs, _looped, first_plan, second_plan = plan
        cfg = (chips, params, total, rows, unit, count, owned, piece, plan)
        pad = lambda n: -(-n // sublanes) * sublanes
        norm_rows = pad(count // lanes + 1)
        dma = pltpu.SemaphoreType.DMA
        return pl.pallas_call(
            functools.partial(kernel, cfg),
            out_shape=jax.ShapeDtypeStruct((owned, count), jnp.float32),
            in_specs=[pl.BlockSpec(memory_space=pl.ANY)] * 2,
            out_specs=pl.BlockSpec(memory_space=pltpu.VMEM),
            scratch_shapes=[
                pltpu.VMEM((count, total), jnp.bfloat16),
                pltpu.VMEM((2 * rows + far, total), jnp.bfloat16),
                pltpu.VMEM((far, total), jnp.bfloat16),
                pltpu.VMEM((2 * rows + far, count), jnp.float32),
                pltpu.VMEM((far, count), jnp.float32),
                pltpu.VMEM((count, lanes), jnp.float32),
                pltpu.VMEM((params, owned, count), jnp.float32),
                pltpu.VMEM((params, norm_rows, lanes), jnp.float32),
                pltpu.VMEM((rows, lanes), jnp.float32),
                pltpu.VMEM((norm_rows, lanes), jnp.float32),
                pltpu.VMEM((norm_rows, lanes), jnp.float32),
                dma((len(first_plan),)),
                dma((len(first_plan),)),
                dma((chips - 1,)),
                dma((chips - 1, len(first_plan))),
                dma((chips - 1, len(second_plan))),
                dma((1,)),
                dma((1,)),
                dma((1,)),
                dma((chips - 1, len(first_plan))),
                dma((chips - 1, len(second_plan))),
                dma((1,)),
                dma((1,)),
                dma((1,)),
                dma((1,)),
                dma((1,)),
                dma((1,)),
                pltpu.SemaphoreType.REGULAR((params // 4,)),
            ],
            compiler_params=pltpu.CompilerParams(
                collective_id=0, has_side_effects=True, vmem_limit_bytes=62 * 1024 * 1024
            ),
        )(train_grads, query_grads)

    return jax.shard_map(
        per_device,
        mesh=mesh,
        in_specs=(P("dp", "param"), P("dp", "param")),
        out_specs=P("param", "dp"),
        check_vma=False,
    )
```

```python
import functools

import jax
import jax.numpy as jnp
from jax import lax
from jax.experimental import pallas as pl
from jax.experimental.pallas import tpu as pltpu
from jax.sharding import PartitionSpec as P

epsilon = 1e-06
lanes = 128
sublanes = 8
max_chunk = 2048
block_rows = 256
train_width = 1024
x_width = 1024


def chunk_width(width):
    best = lanes
    for tiles in range(1, max_chunk // lanes + 1):
        if width % (tiles * lanes) == 0:
            best = tiles * lanes
    return best


def column_plan(total):
    base = chunk_width(total)
    chunks = total // base
    pairs = (chunks - 1) // 2
    first = [(2 * base * g, 2 * base) for g in range(pairs)]
    first.append((2 * base * pairs, total - 2 * base * pairs))
    looped = max(chunks - 2, 0)
    second = [(base * c, base) for c in range(looped)]
    fine = 1024 if base % 1024 == 0 else base
    second += [(at, fine) for at in range(base * looped, total, fine)]
    return base, pairs, looped, first, second


def nt_dot(a, b):
    return lax.dot_general(a, b, (((1,), (1,)), ((), ())), preferred_element_type=jnp.float32)


def kernel(
    cfg, train_hbm, query_hbm, out_ref,
    train, first_q, second_q, first_sum, second_sum, norm_sum, parts, norm_parts, query_sum, query_scales, scale,
    train_sem, self_sem, x_send, first_recv, second_recv, mate_send, mate_recv,
    fwd_send, first_fwd, second_fwd, part_send, part_recv, norm_send, norm_recv,
    query_send, query_recv, known,
):
    chips, params, total, rows, unit, count, owned, piece, plan = cfg
    base, pairs, looped, first_plan, second_plan = plan
    dp = lax.axis_index("dp")
    me = lax.axis_index("param")
    chip, core = dp // 2, lax.rem(dp, 2)
    mate = chip * 2 + (1 - core)
    cores = 2 * chips
    near = 2 * rows
    x_recv = (first_recv, second_recv)
    fwd_recv = (first_fwd, second_fwd)

    def bytes_wait(ref, sem):
        pltpu.make_async_copy(ref, ref, sem).wait()

    def columns(group, i):
        plan_of = first_plan if group == 0 else second_plan
        if isinstance(i, int):
            start, size = plan_of[i]
            return pl.ds(start, size)
        width = 2 * base if group == 0 else base
        return pl.ds(pl.multiple_of(i * width, width), width)

    def split(start, size, width):
        return [pl.ds(start + k, min(width, size - k)) for k in range(0, size, width)]

    def train_copies(i):
        return [
            pltpu.make_async_copy(train_hbm.at[:, cols], train.at[:, cols], train_sem.at[i])
            for cols in split(*first_plan[i], train_width)
        ]

    def self_copies(i):
        return [
            pltpu.make_async_copy(query_hbm.at[:, cols], first_q.at[pl.ds(0, rows), cols], self_sem.at[i])
            for cols in split(*first_plan[i], base)
        ]

    def wait_train(i):
        bytes_wait(query_hbm.at[:, columns(0, i)], self_sem.at[i])
        bytes_wait(train.at[:, columns(0, i)], train_sem.at[i])

    def mate_copies(i):
        return [
            pltpu.make_async_remote_copy(
                src_ref=query_hbm.at[:, cols],
                dst_ref=first_q.at[pl.ds(rows, rows), cols],
                send_sem=mate_send.at[0],
                recv_sem=mate_recv.at[0],
                device_id={"dp": mate},
            )
            for cols in split(*first_plan[i], base)
        ]

    def slot(group, i, place):
        if group == 0:
            return first_q.at[pl.ds(near + unit * place, unit), columns(0, i)]
        return second_q.at[pl.ds(unit * place, unit), columns(1, i)]

    def x_copies(group, i, d):
        start = pl.multiple_of(lax.rem(group + core, 2) * unit, unit)
        place = pl.ds((near if group == 0 else 0) + unit * 2 * (d - 1), unit)
        dst = first_q if group == 0 else second_q
        return [
            pltpu.make_async_remote_copy(
                src_ref=query_hbm.at[pl.ds(start, unit), cols],
                dst_ref=dst.at[place, cols],
                send_sem=x_send.at[d - 1],
                recv_sem=x_recv[group].at[d - 1, i],
                device_id={"dp": lax.rem(chip + d, chips) * 2 + core},
            )
            for cols in split(*(first_plan if group == 0 else second_plan)[i], x_width)
        ]

    def fwd_copy(group, i, d):
        return pltpu.make_async_remote_copy(
            src_ref=slot(group, i, 2 * (d - 1)),
            dst_ref=slot(group, i, 2 * (d - 1) + 1),
            send_sem=fwd_send.at[0],
            recv_sem=fwd_recv[group].at[d - 1, i],
            device_id={"dp": mate},
        )

    def pump(group, i):
        for d in range(1, chips):
            bytes_wait(slot(group, i, 2 * (d - 1)), x_recv[group].at[d - 1, i])
            fwd_copy(group, i, d).start()

    def arrive(group, i):
        for d in range(1, chips):
            fwd_copy(group, i, d).wait_recv()

    def piece_list(group):
        out = []
        if group == 0:
            for source, at in ((dp, 0), (mate, rows)):
                for r in range(0, rows, piece):
                    out.append((first_sum, at + r, source * rows + r))
        for d in range(1, chips):
            other = lax.rem(chip - d + chips, chips)
            for k in range(2):
                from_core = core if k == 0 else 1 - core
                start = lax.rem(group + from_core, 2) * unit
                at = unit * (2 * (d - 1) + k)
                for r in range(0, unit, piece):
                    row = (other * 2 + from_core) * rows + start + r
                    if group == 0:
                        out.append((first_sum, near + at + r, row))
                    else:
                        out.append((second_sum, at + r, row))
        return out

    def send_parts(items):
        for buffer, at, row in items:
            owner, offset = row // owned, lax.rem(row, owned)
            place = parts.at[me, pl.ds(pl.multiple_of(offset, piece), piece), :]
            copy = pltpu.make_async_remote_copy(
                src_ref=buffer.at[pl.ds(at, piece), :],
                dst_ref=place,
                send_sem=part_send.at[0],
                recv_sem=part_recv.at[0],
                device_id={"param": owner},
            )

            @pl.when(owner != me)
            def _():
                copy.start()

            @pl.when(owner == me)
            def _():
                place[...] = buffer[pl.ds(at, piece), :]

    def norm_copy(j):
        return pltpu.make_async_remote_copy(
            src_ref=norm_parts.at[me],
            dst_ref=norm_parts.at[me],
            send_sem=norm_send.at[0],
            recv_sem=norm_recv.at[0],
            device_id={"param": lax.rem(me + j, params)},
        )

    def query_copy(j):
        return pltpu.make_async_remote_copy(
            src_ref=query_scales,
            dst_ref=query_scales,
            send_sem=query_send.at[0],
            recv_sem=query_recv.at[0],
            device_id={"dp": lax.rem(dp + j, cores)},
        )

    pairmate = me + 1 - 2 * lax.rem(me, 2)
    neighbours = (pairmate, lax.rem(me + 2, params), lax.rem(me + params - 2, params))
    stages = known.shape[0]

    for i in range(len(first_plan)):
        for copy in self_copies(i) + train_copies(i):
            copy.start()

    barrier = pltpu.get_barrier_semaphore()
    for j in range(1, cores):
        pl.semaphore_signal(barrier, inc=1, device_id={"dp": lax.rem(dp + j, cores)})
    for other in neighbours:
        pl.semaphore_signal(barrier, inc=1, device_id={"param": other})
    pl.semaphore_wait(barrier, cores - 1 + len(neighbours))

    for other in neighbours:
        pl.semaphore_signal(known.at[0], inc=1, device_id={"param": other})
    for i in range(len(first_plan)):
        for d in range(1, chips):
            for copy in x_copies(0, i, d):
                copy.start()
        for copy in mate_copies(i):
            copy.start()
    for i in range(len(second_plan)):
        for d in range(1, chips):
            for copy in x_copies(1, i, d):
                copy.start()

    first_sum[...] = jnp.zeros_like(first_sum)
    second_sum[...] = jnp.zeros_like(second_sum)
    norm_sum[...] = jnp.zeros_like(norm_sum)

    query_sum[...] = jnp.zeros_like(query_sum)

    def next_round(stage):
        pl.semaphore_wait(known.at[stage], len(neighbours))
        if stage + 1 < stages:
            for other in neighbours:
                pl.semaphore_signal(known.at[stage + 1], inc=1, device_id={"param": other})

    def multiply(sums, q_ref, start, width, norms):
        if not isinstance(start, int):
            start = pl.multiple_of(start, base)
        q = q_ref[:, pl.ds(start, width)]
        if norms:
            acc = query_sum[...]
            for k in range(0, width, lanes):
                x = q[:rows, k : k + lanes].astype(jnp.float32)
                acc = acc + x * x
            query_sum[...] = acc
        for r in range(0, count, block_rows):
            size = min(block_rows, count - r)
            t = train[pl.ds(r, size), pl.ds(start, width)]
            sums[:, pl.ds(r, size)] += nt_dot(q, t)
            if norms:
                for s in range(0, size, lanes):
                    acc = norm_sum[pl.ds(r + s, lanes), :]
                    for k in range(0, width, lanes):
                        x = t[s : s + lanes, k : k + lanes].astype(jnp.float32)
                        acc = acc + x * x
                    norm_sum[pl.ds(r + s, lanes), :] = acc

    bytes_wait(query_hbm, mate_recv.at[0])
    pump(0, 0)

    @pl.loop(0, pairs)
    def _(g):
        wait_train(g)
        arrive(0, g)
        multiply(first_sum, first_q, g * 2 * base, base, True)

        @pl.when(g + 1 < pairs)
        def _():
            pump(0, g + 1)

        @pl.when(g + 1 == pairs)
        def _():
            pump(0, pairs)

        multiply(first_sum, first_q, g * 2 * base + base, base, True)

        @pl.when(g == 0)
        def _():
            next_round(0)

    start, size = first_plan[pairs]
    wait_train(pairs)
    arrive(0, pairs)
    for at in range(start, start + size, base):
        multiply(first_sum, first_q, at, base, True)

    for stage in range(1, stages):
        next_round(stage)
    send_parts(piece_list(0))

    totals = [
        jnp.sum(norm_sum[pl.ds(r, lanes), :].T, axis=0, keepdims=True) for r in range(0, count, lanes)
    ]
    query_row = len(totals)
    square = jnp.concatenate([query_sum[...], jnp.zeros((lanes - rows, lanes), jnp.float32)], axis=0)
    totals.append(jnp.sum(square.T, axis=0, keepdims=True))
    spare = norm_parts.shape[1] - len(totals)
    if spare:
        totals.append(jnp.zeros((spare, lanes), jnp.float32))
    norm_parts[me] = jnp.concatenate(totals, axis=0)
    for j in range(1, params):
        norm_copy(j).start()

    first_row = me * owned
    source = first_row // rows

    def share_scales():
        bytes_wait(norm_parts.at[pl.ds(0, params - 1)], norm_send.at[0])
        bytes_wait(norm_parts.at[pl.ds(0, params - 1)], norm_recv.at[0])
        norm = norm_parts[0]
        for j in range(1, params):
            norm = norm + norm_parts[j]
        scale[...] = lax.rsqrt(norm + epsilon)

        @pl.when(dp == source)
        def _():
            query_scales[...] = jnp.broadcast_to(scale[query_row : query_row + 1, :], query_scales.shape)
            for j in range(1, cores):
                query_copy(j).start()

    pump(1, 0)
    if looped:
        @pl.loop(0, looped)
        def _(c):
            @pl.when(c + 1 < looped)
            def _():
                pump(1, c + 1)

            @pl.when(c + 1 == looped)
            def _():
                pump(1, looped)

            arrive(1, c)
            multiply(second_sum, second_q, c * base, base, False)

            @pl.when(c == max(looped - 3, 0))
            def _():
                share_scales()

    else:
        share_scales()

    last = len(second_plan) - 1
    if looped < last:
        pump(1, looped + 1)
    for i in range(looped, last + 1):
        if i + 2 <= last:
            pump(1, i + 2)
        arrive(1, i)
        multiply(second_sum, second_q, *second_plan[i], False)

    send_parts(piece_list(1))

    @pl.when(dp == source)
    def _():
        bytes_wait(norm_parts.at[pl.ds(0, cores - 1)], query_send.at[0])

    @pl.when(dp != source)
    def _():
        bytes_wait(query_scales, query_recv.at[0])

    pick = lax.broadcasted_iota(jnp.int32, (owned, lanes), 1) == (
        lax.broadcasted_iota(jnp.int32, (owned, lanes), 0) + lax.rem(first_row, rows)
    )
    query_scale = jnp.sum(jnp.where(pick, query_scales[0:1, :], 0.0), axis=1, keepdims=True)

    bytes_wait(query_hbm, mate_send.at[0])
    for d in range(1, chips):
        bytes_wait(query_hbm, x_send.at[d - 1])
    bytes_wait(second_q, fwd_send.at[0])

    bytes_wait(parts.at[pl.ds(0, params - 1)], part_recv.at[0])
    for k in range(count // lanes):
        at = slice(k * lanes, (k + 1) * lanes)
        products = parts[0, :, at]
        for j in range(1, params):
            products = products + parts[j, :, at]
        out_ref[:, at] = products * query_scale * scale[k : k + 1, :]

    bytes_wait(parts.at[pl.ds(0, params - 1)], part_send.at[0])


def solution(mesh):
    chips, params = mesh.shape["dp"] // 2, mesh.shape["param"]

    def per_device(train_grads, query_grads):
        count, total = train_grads.shape
        rows = query_grads.shape[0]
        unit = rows // 2
        cores = 2 * chips
        owned = rows * cores // params
        piece = min(unit, owned)
        far = 2 * (chips - 1) * unit
        plan = column_plan(total)
        _base, _pairs, _looped, first_plan, second_plan = plan
        cfg = (chips, params, total, rows, unit, count, owned, piece, plan)
        pad = lambda n: -(-n // sublanes) * sublanes
        norm_rows = pad(count // lanes + 1)
        dma = pltpu.SemaphoreType.DMA
        return pl.pallas_call(
            functools.partial(kernel, cfg),
            out_shape=jax.ShapeDtypeStruct((owned, count), jnp.float32),
            in_specs=[pl.BlockSpec(memory_space=pl.ANY)] * 2,
            out_specs=pl.BlockSpec(memory_space=pltpu.VMEM),
            scratch_shapes=[
                pltpu.VMEM((count, total), jnp.bfloat16),
                pltpu.VMEM((2 * rows + far, total), jnp.bfloat16),
                pltpu.VMEM((far, total), jnp.bfloat16),
                pltpu.VMEM((2 * rows + far, count), jnp.float32),
                pltpu.VMEM((far, count), jnp.float32),
                pltpu.VMEM((count, lanes), jnp.float32),
                pltpu.VMEM((params, owned, count), jnp.float32),
                pltpu.VMEM((params, norm_rows, lanes), jnp.float32),
                pltpu.VMEM((rows, lanes), jnp.float32),
                pltpu.VMEM((norm_rows, lanes), jnp.float32),
                pltpu.VMEM((norm_rows, lanes), jnp.float32),
                dma((len(first_plan),)),
                dma((len(first_plan),)),
                dma((chips - 1,)),
                dma((chips - 1, len(first_plan))),
                dma((chips - 1, len(second_plan))),
                dma((1,)),
                dma((1,)),
                dma((1,)),
                dma((chips - 1, len(first_plan))),
                dma((chips - 1, len(second_plan))),
                dma((1,)),
                dma((1,)),
                dma((1,)),
                dma((1,)),
                dma((1,)),
                dma((1,)),
                pltpu.SemaphoreType.REGULAR((params // 4,)),
            ],
            compiler_params=pltpu.CompilerParams(
                collective_id=0, has_side_effects=True, vmem_limit_bytes=62 * 1024 * 1024
            ),
        )(train_grads, query_grads)

    return jax.shard_map(
        per_device,
        mesh=mesh,
        in_specs=(P("dp", "param"), P("dp", "param")),
        out_specs=P("param", "dp"),
        check_vma=False,
    )
```
